32 devices in a mesh: inner: 4 (over x, core), outer: 8 (over z, y).
Axes of the slice: x: 2, y: 2, z: 4, core: 2. Of those that a mesh axis runs over, the one named last changes fastest.
Arguments:
- tokens: bfloat16 [4096, 4096], P(('inner', 'outer')), may hold values from -6 to 6
- weight_codes: bfloat16 [4096, 512], P('inner'), may hold values from -127 to 127
- scales: float32 [1024], P('inner'), may hold values from 0.00012 to 0.0004
- cotangent: bfloat16 [4096, 512], P(('inner', 'outer')), may hold values from -6 to 6
Outputs:
- keys: bfloat16 [4096, 512], P(('inner', 'outer'))
- grad_tokens: bfloat16 [4096, 4096], P(('inner', 'outer'))
- grad_weight: float32 [4096, 512], P(('inner', 'outer'))
The draws below stay inside these ranges and needn't reach their ends.
All inputs are finite; a program needn't handle non-finite values.
Results may differ from the reference program's by a relative error of at most 0.017.
Values may be sent and summed in bfloat16 or wider, within the bound.
No kernel may reach another device: no remote copies, remote signals or barrier semaphores. Data moves between devices by JAX's collectives and lax.ppermute only.
A program may use at most 64 MiB of HBM per device.

```python
import math
import jax
import jax.numpy as jnp
from jax import lax

D = 4096
TOK_DEV = 128
KV = 512
QROWS = 4
TOKENS = 4096
N_INNER = 4
N_OUTER = 8


def spiked(values, rng, source, target, parts, factor):
    def block_of(dim):
        return (jnp.arange(values.shape[dim]) // (values.shape[dim] // parts)).reshape((-1,) + (1,) * (values.ndim - 1 - dim))

    first = jax.random.permutation(rng, parts)[block_of(target)]
    second = (block_of(target) + parts // 2) % parts
    return jnp.where((block_of(source) == first) | (block_of(source) == second), factor * values, values)


def block_scale(rng, dims, split, low, largest):
    factor_of, own = 1.0, jax.random.fold_in(rng, 6)
    for position, blocks in split:
        steps = jnp.exp(jax.random.uniform(jax.random.fold_in(own, position), (blocks,), jnp.float32, low / len(split), largest / len(split)))
        factor_of = factor_of * jnp.repeat(steps, dims[position] // blocks).reshape([-1 if axis == position else 1 for axis in range(len(dims))])
    return factor_of


def centred(own_key, shape, spread, most, shards=(), kind=jnp.bfloat16):
    result = spread * jax.random.normal(own_key, shape, jnp.float32)
    if shards:
        result = result * block_scale(own_key, shape, shards, -0.22, 0.18)
    return jnp.clip(result, -most, most).astype(kind)


def bell_draw_with(rng, extent, scale, bound, shards, heavy, dtype=jnp.bfloat16):
    array = scale * jax.random.normal(rng, extent, jnp.float32)
    if shards:
        array = array * block_scale(rng, extent, shards, -0.22, 0.18)
    return jnp.clip(spiked(array, jax.random.fold_in(rng, 3), *heavy), -bound, bound).astype(dtype)


def setup_inputs(seed: int = 0) -> dict:
    key_of = jax.random.split(jax.random.key(seed), 5)
    tokens = bell_draw_with(key_of[0], (TOKENS, D), 1.0, 6.0, ((0, 32),), (0, 1, 32, 2.75))
    weight_codes = jnp.clip(jax.random.uniform(key_of[1], (D, KV), jnp.float32, -127.0, 127.0) * block_scale(key_of[1], (D, KV), ((0, 4),), -0.4, 0.0), -127.0, 127.0).astype(jnp.bfloat16)
    scales = jnp.clip(jnp.exp(math.log(0.0004) - 1.2039728 * jax.random.uniform(key_of[2], (D // QROWS,), jnp.float32) ** block_scale(key_of[2], (D // QROWS,), ((0, 4),), -0.2, 0.2)), 0.00012, 0.0004)
    cotangent = centred(key_of[3], (TOKENS, KV), 1.0, 6.0, ((0, 32),))
    return dict(tokens=tokens, weight_codes=weight_codes, scales=scales, cotangent=cotangent)


EPS = 1e-05

def block_pass(block_x, block_ct, weight):
    xf = block_x.astype(jnp.float32)
    inv_norm = lax.rsqrt(lax.optimization_barrier(jnp.mean(xf * xf, axis=-1, keepdims=True)) + EPS)
    normed_f = xf * inv_norm
    normed = normed_f.astype(jnp.bfloat16)
    keys = jnp.dot(normed, weight, preferred_element_type=jnp.float32).astype(jnp.bfloat16)
    grad_normed = lax.dot_general(block_ct, weight, (((1,), (1,)), ((), ())), preferred_element_type=jnp.float32)
    inner_mean = lax.optimization_barrier(jnp.mean(grad_normed * normed_f, axis=-1, keepdims=True))
    grad_x = (inv_norm * (grad_normed - normed_f * inner_mean)).astype(jnp.bfloat16)
    partial_value = lax.dot_general(normed, block_ct, (((0,), (0,)), ((), ())), preferred_element_type=jnp.float32)
    partial_value = lax.optimization_barrier(partial_value.astype(jnp.bfloat16)).astype(jnp.float32)
    return (keys, grad_x, partial_value)

def reference(tokens, weight_codes, scales, cotangent):
    devices_all = N_INNER * N_OUTER
    scaled = weight_codes.astype(jnp.float32).reshape(D // QROWS, QROWS * KV) * scales[:, None]
    weight = scaled.reshape(D, KV).astype(jnp.bfloat16)
    blocks_x = tokens.reshape(devices_all, TOK_DEV, D)
    blocks_ct = cotangent.reshape(devices_all, TOK_DEV, KV)

    def stepper(total, pair):
        keys, grad_x, partial_value = block_pass(pair[0], pair[1], weight)
        return (total + partial_value, (keys, grad_x))
    start_total = jnp.zeros((D, KV), jnp.float32)
    grad_weight, outs = lax.scan(stepper, start_total, (blocks_x, blocks_ct))
    keys = outs[0].reshape(TOKENS, KV)
    grad_tokens = outs[1].reshape(TOKENS, D)
    return (keys, grad_tokens, grad_weight)
```

```python
import functools

import jax
import jax.numpy as jnp
from jax import lax
from jax.experimental import pallas as pl
from jax.experimental.pallas import tpu as pltpu
from jax.sharding import PartitionSpec as P

EPS = 1e-05
LANES = 128
F32, BF16 = jnp.float32, jnp.bfloat16
VMEM = pl.BlockSpec(memory_space=pltpu.VMEM)
SMEM = pl.BlockSpec(memory_space=pltpu.SMEM)


def call(body, ins, outs, smem=0, flops=0, limit=24):
    specs = [SMEM] * smem + [VMEM] * (len(ins) - smem)
    moved = sum(a.size * a.dtype.itemsize for a in [*ins, *outs])
    return pl.pallas_call(
        body,
        out_shape=outs,
        in_specs=specs,
        out_specs=[VMEM] * len(outs),
        cost_estimate=pl.CostEstimate(flops=max(flops, 4 * moved), bytes_accessed=moved, transcendentals=0),
        compiler_params=pltpu.CompilerParams(vmem_limit_bytes=limit * 1024 * 1024),
    )(*ins)


def dot(a, b, ca, cb):
    return lax.dot_general(a, b, (((ca,), (cb,)), ((), ())), preferred_element_type=F32)


def norm_body(n, m, width, pos, x_ref, inv_ref, *outs):
    x = x_ref[...].astype(F32)
    inv = lax.rsqrt(jnp.mean(x * x, axis=-1, keepdims=True) + EPS)
    inv_ref[...] = jnp.broadcast_to(inv, inv_ref.shape)
    for r in range(n):
        for c in range(2):
            for z in range(m // 2):
                block = (pos[0] ^ r) * m + 2 * z + (pos[1] ^ (1 - c))
                src = pl.multiple_of(block * width, LANES)
                piece = x_ref[:, pl.ds(src, width)].astype(F32) * inv
                outs[2 * r + c][:, z * width : (z + 1) * width] = piece.astype(BF16)


def weight_body(m, width, pos, codes_ref, scales_ref, out_ref):
    rows, groups = codes_ref.shape[0], scales_ref.shape[1]
    per = rows // groups
    for c in range(2):
        for z in range(m // 2):
            block = 2 * z + (pos[1] ^ (1 - c))
            src = pl.multiple_of(block * width, width)
            row = (lax.broadcasted_iota(jnp.int32, (width, groups), 0) + src) // per
            hit = row == lax.broadcasted_iota(jnp.int32, (width, groups), 1)
            scale = jnp.sum(jnp.where(hit, scales_ref[...], 0.0), axis=1, keepdims=True)
            to = (c * (m // 2) + z) * width
            out_ref[to : to + width, :] = (codes_ref[pl.ds(src, width), :].astype(F32) * scale).astype(BF16)


def grad_body(n, w_ref, *refs):
    for ct, out in zip(refs[:n], refs[n:]):
        out[...] = dot(ct[...], w_ref[...], 1, 1).astype(BF16)


def part_body(n, *refs):
    normed, cts, out = refs[:n], refs[n : 2 * n], refs[2 * n]
    total = dot(normed[0][...], cts[0][...], 0, 0)
    for a, b in zip(normed[1:], cts[1:]):
        total += dot(a[...], b[...], 0, 0)
    out[...] = total.astype(out.dtype)


def keys_body(n, w_ref, *refs):
    half = w_ref.shape[0] // 2
    for r in range(n):
        a = dot(refs[2 * r][...], w_ref[:half, :], 1, 0) + dot(refs[2 * r + 1][...], w_ref[half:, :], 1, 0)
        refs[2 * n + r][...] = a.astype(refs[2 * n + r].dtype)


def fold_body(width, k, pos, mine_ref, got_ref, own_ref, *outs):
    for r in range(k):
        at = pl.ds(pl.multiple_of((pos[2] ^ r) * width, width), width)
        total = mine_ref[at, :] + got_ref[at, :].astype(F32)
        if r == 0:
            own_ref[...] = total
        else:
            outs[r - 1][...] = total.astype(BF16)


def sum_body(*refs):
    total = refs[0][...].astype(F32)
    for a in refs[1:-1]:
        total += a[...].astype(F32)
    refs[-1][...] = total.astype(refs[-1].dtype)


def finish_body(n, m, width, pos, x_ref, inv_ref, *refs):
    gns, out = refs[:n], refs[n]
    inv = inv_ref[:, :1]
    total = jnp.zeros((x_ref.shape[0], width), F32)

    def place(r, c, z):
        block = (pos[0] ^ r) * m + 2 * z + (pos[1] ^ (1 - c))
        src = pl.ds(pl.multiple_of(block * width, LANES), width)
        at = (c * (m // 2) + z) * width
        return src, gns[r][:, at : at + width].astype(F32)

    every = [(r, c, z) for r in range(n) for c in range(2) for z in range(m // 2)]
    for r, c, z in every:
        src, gn = place(r, c, z)
        total += gn * (x_ref[:, src].astype(F32) * inv)
    mean = jnp.sum(total, axis=-1, keepdims=True) / x_ref.shape[1]
    for r, c, z in every:
        src, gn = place(r, c, z)
        out[:, src] = (inv * (gn - x_ref[:, src].astype(F32) * inv * mean)).astype(BF16)


def direct(n, m, tokens, codes, scales, ct):
    toks, feats = tokens.shape
    kv = ct.shape[1]
    rows = codes.shape[0]
    width, k = rows // m, m // 2
    i, o = lax.axis_index("inner"), lax.axis_index("outer")
    pos = jnp.stack([i, o % 2, o // 2]).astype(jnp.int32)
    sds = jax.ShapeDtypeStruct

    def inner(a, r):
        return lax.ppermute(a, "inner", [(s, s ^ r) for s in range(n)])

    def outer(a, r):
        return lax.ppermute(a, "outer", [(s, s ^ r) for s in range(m)])

    cts = [ct] + [None] * (n - 1)
    for r in range(2, n, 2):
        cts[r] = inner(ct, r)
    inv, *normed = call(
        functools.partial(norm_body, n, m, width),
        [pos, tokens],
        [sds((toks, LANES), F32)] + [sds((toks, k * width), BF16)] * (2 * n),
        smem=1,
    )
    for r in range(0, n, 2):
        cts[r + 1] = inner(cts[r], 1)
    got = [[normed[c]] + [inner(normed[2 * r + c], r) for r in range(1, n)] for c in range(2)]
    (weight,) = call(
        functools.partial(weight_body, m, width), [pos, codes, scales[None, :]], [sds((rows, kv), BF16)], smem=1
    )
    gns = call(
        functools.partial(grad_body, n),
        [weight, *cts],
        [sds((toks, rows), BF16)] * n,
        flops=2 * n * toks * kv * rows,
    )
    flops = 2 * n * toks * kv * rows // 2
    (far,) = call(functools.partial(part_body, n), [*got[0], *cts], [sds((rows // 2, kv), BF16)], flops=flops)
    far = outer(far, 1)
    (near,) = call(functools.partial(part_body, n), [*got[1], *cts], [sds((rows // 2, kv), F32)], flops=flops)
    both = [got[c][r] for r in range(n) for c in range(2)]
    keys = call(
        functools.partial(keys_body, n),
        [weight, *both],
        [sds((toks, kv), F32)] + [sds((toks, kv), BF16)] * (n - 1),
        flops=2 * flops,
    )
    own, *rest = call(
        functools.partial(fold_body, width, k),
        [pos, near, far],
        [sds((width, kv), F32)] + [sds((width, kv), BF16)] * (k - 1),
        smem=1,
    )
    rest = [outer(a, 2 * r) for r, a in enumerate(rest, 1)]
    gns = [gns[0]] + [inner(gns[r], r) for r in range(1, n)]
    keys = [keys[0]] + [inner(keys[r], r) for r in range(1, n)]
    (grad_weight,) = call(sum_body, [own, *rest], [sds((width, kv), F32)])
    (keys,) = call(sum_body, keys, [sds((toks, kv), BF16)])
    (grad_tokens,) = call(
        functools.partial(finish_body, n, m, width), [pos, tokens, inv, *gns], [sds((toks, feats), BF16)], smem=1
    )
    return keys, grad_tokens, grad_weight


def gathered(tokens, weight_codes, scales, cotangent):
    kv_width = cotangent.shape[1]
    tok_rows = tokens.shape[0]
    xf = tokens.astype(F32)
    inv_norm = lax.rsqrt(jnp.mean(xf * xf, axis=-1, keepdims=True) + EPS)
    normed_f = xf * inv_norm
    normed = normed_f.astype(BF16)
    scale = jnp.repeat(scales, weight_codes.shape[0] // scales.shape[0])
    piece = (weight_codes.astype(F32) * scale[:, None]).astype(BF16)
    weight = lax.all_gather(piece, "inner", axis=0, tiled=True)
    keys = jnp.dot(normed, weight, preferred_element_type=F32).astype(BF16)
    grad_normed = dot(cotangent, weight, 1, 1)
    slab = lax.all_to_all(normed, "inner", split_axis=1, concat_axis=0, tiled=True)
    grads = lax.all_gather(cotangent, "inner", axis=0, tiled=True)
    grad_weight = lax.psum_scatter(dot(slab, grads, 0, 0), "outer", scatter_dimension=0, tiled=True)
    inner_mean = jnp.mean(grad_normed * normed_f, axis=-1, keepdims=True)
    grad_tokens = (inv_norm * (grad_normed - normed_f * inner_mean)).astype(BF16)
    return keys, grad_tokens, grad_weight


def solution(mesh):
    n, m = mesh.shape["inner"], mesh.shape["outer"]

    def local(tokens, weight_codes, scales, cotangent):
        width = weight_codes.shape[0] // m
        powers = n & (n - 1) == 0 and m & (m - 1) == 0
        if powers and 2 <= n <= 8 and 2 <= m <= 16 and width % LANES == 0:
            return direct(n, m, tokens, weight_codes, scales, cotangent)
        return gathered(tokens, weight_codes, scales, cotangent)

    in_specs = (
        P(("inner", "outer"), None),
        P("inner", None),
        P("inner"),
        P(("inner", "outer"), None),
    )
    out_specs = (P(("inner", "outer"), None),) * 3
    return jax.shard_map(local, mesh=mesh, in_specs=in_specs, out_specs=out_specs, check_vma=False)
```
